32 devices in a mesh: shift: 2 (over y), expert: 4 (over z), shard: 4 (over x, core).
Axes of the slice: x: 2, y: 2, z: 4, core: 2. Of those that a mesh axis runs over, the one named last changes fastest.
Arguments:
- master_gate: float32 [128, 2048, 1024], P(('shift', 'expert'), 'shard'), parts along dimension 0, may hold values from -0.1875 to 0.1875
- master_up: float32 [128, 2048, 1024], P(('shift', 'expert'), 'shard'), parts along dimension 0, may hold values from -0.1875 to 0.1875
- router_weight: float32 [4096, 64], P(('shift', 'shard'), 'expert'), parts along dimension 0, may hold values from -0.125 to 0.125
- router_gain: float32 [4096], P(('shift', 'shard')), parts along dimension 0, may hold values from 0.25 to 1.75
Outputs:
- final_gate: bfloat16 [128, 2048, 1024], P(('shift', 'expert'), None, 'shard'), parts along dimension 0
- final_up: bfloat16 [128, 2048, 1024], P(('shift', 'expert'), None, 'shard'), parts along dimension 0
- scale_gate: float32 [128, 1024], P(('shift', 'expert'), 'shard'), parts along dimension 0
- scale_up: float32 [128, 1024], P(('shift', 'expert'), 'shard'), parts along dimension 0
- serve_router: bfloat16 [4096, 64], P('shift'), parts along dimension 0
The draws below stay inside these ranges and needn't reach their ends.
There are 2 independent parts, one for each index of `shift`. The reference program is written for one: setup_inputs(seed, part) draws one part's arguments, and reference() takes and returns one part's arrays. A program takes and returns all parts, laid end to end along the dimension named above; each array names one. Nothing has to cross between parts.
All inputs are finite; a program needn't handle non-finite values. Where the reference program divides by a largest or mean magnitude, that divisor is 1e-20 or more.
Results may differ from the reference program's by a relative error of at most 0.001.
Values may be sent and summed in bfloat16 or wider, within the bound.
No kernel may reach another device: no remote copies, remote signals or barrier semaphores. Data moves between devices by JAX's collectives and lax.ppermute only.
A program may use at most 256 MiB of HBM per device.

```python
import jax
import jax.numpy as jnp

EXPERTS = 64
D_MODEL = 2048
D_EXPERT = 1024


def spiked(values, rng, source, target, blocks, factor):
    def block_of(axis_at):
        return (jnp.arange(values.shape[axis_at]) // (values.shape[axis_at] // blocks)).reshape((-1,) + (1,) * (values.ndim - 1 - axis_at))

    first = jax.random.permutation(rng, blocks)[block_of(target)]
    second = (block_of(target) + blocks // 2) % blocks
    return jnp.where((block_of(source) == first) | (block_of(source) == second), factor * values, values)


def block_levels(stream_key, shape, split, smallest, high):
    gain = 1.0
    for dim, shards_of in split:
        steps = jax.random.uniform(jax.random.fold_in(jax.random.fold_in(stream_key, 6), dim), (shards_of,), jnp.float32, smallest / len(split), high / len(split))
        gain = gain * jnp.repeat(jnp.exp(steps), shape[dim] // shards_of).reshape((-1,) + (1,) * (len(shape) - 1 - dim))
    return gain


def bell_draw(rng, shape, width, reach, cuts=(), held_as=jnp.bfloat16):
    values = jax.random.normal(rng, shape, jnp.float32) * width
    if len(cuts) > 0:
        values = block_levels(rng, shape, cuts, -0.22, 0.18) * values
    return jnp.clip(values, min=-reach, max=reach).astype(held_as)


def bell_draw_with(stream_key, dims, spread, most, pieces, heavy, kind=jnp.bfloat16):
    array = spread * jax.random.normal(stream_key, dims, jnp.float32)
    if pieces:
        array = array * block_levels(stream_key, dims, pieces, -0.22, 0.18)
    return jnp.clip(spiked(array, jax.random.fold_in(stream_key, 3), *heavy), -most, most).astype(kind)


def setup_inputs(seed: int = 0, part: int = 0) -> dict:
    seeds = jax.random.split(jax.random.key(seed), 5)
    part_splits = jax.random.split(jax.random.fold_in(seeds[4], part), 5)
    master_gate = bell_draw_with(part_splits[0], (EXPERTS, D_MODEL, D_EXPERT), D_MODEL ** -0.5, 0.1875, ((0, 4), (1, 4)), (1, 2, 4, 2.0), jnp.float32)
    master_up = bell_draw_with(part_splits[1], (EXPERTS, D_MODEL, D_EXPERT), D_MODEL ** -0.5, 0.1875, ((0, 4), (1, 4)), (1, 2, 4, 2.0), jnp.float32)
    router_weight = bell_draw(part_splits[2], (D_MODEL, EXPERTS), D_MODEL ** -0.5, 0.125, ((0, 4), (1, 4)), jnp.float32)
    router_gain = jnp.clip(1.0 + 0.15 * jax.random.normal(part_splits[3], (D_MODEL,), jnp.float32), 0.25, 1.75)
    return dict(master_gate=master_gate, master_up=master_up, router_weight=router_weight, router_gain=router_gain)


def reference(master_gate, master_up, router_weight, router_gain):
    scale_gate = jnp.max(jnp.abs(master_gate), axis=1)
    final_gate = (master_gate / jnp.expand_dims(scale_gate, 1)).astype(jnp.bfloat16)
    scale_up = jnp.max(jnp.abs(master_up), axis=1)
    final_up = (master_up / jnp.expand_dims(scale_up, 1)).astype(jnp.bfloat16)
    serve_router = (router_weight * router_gain[:, None]).astype(jnp.bfloat16)
    return final_gate, final_up, scale_gate, scale_up, serve_router
```

```python
import functools

import jax
import jax.numpy as jnp
from jax import lax
from jax.experimental import pallas as pl
from jax.experimental.pallas import tpu as pltpu
from jax.sharding import PartitionSpec as P

LANES = 128
PLAN = [(0, 0, 1), (0, 1, 3), (0, 4, 1), (0, 5, 3), (0, 8, 8), (1, 0, 8), (1, 8, 7), (1, 15, 1)]
LEAD = 3
HBM = pl.BlockSpec(memory_space=pl.ANY)


def swap(value, axis, size, step):
    return lax.ppermute(value, axis, [(i, i ^ step) for i in range(size)])


def peak_body(*refs):
    refs[-1][0] = jnp.max(jnp.abs(refs[0][0]), axis=0, keepdims=True)


def peaks(master, first, count, after=()):
    _, rows, cols = master.shape
    return pl.pallas_call(
        peak_body,
        grid=(count,),
        in_specs=[pl.BlockSpec((1, rows, cols), lambda e: (first + e, 0, 0))] + [HBM] * len(after),
        out_specs=pl.BlockSpec((1, 1, cols), lambda e: (e, 0, 0)),
        out_shape=jax.ShapeDtypeStruct((count, 1, cols), jnp.float32),
        name="peaks",
    )(master, *after)


def narrow_body(n, targets, *refs):
    outs = refs[-n:]
    for d in range(n):
        outs[d][0] = (refs[d][0] / refs[n + d][0]).astype(jnp.bfloat16)


def narrow(master, scale, targets, first, count, offset, n, final=None):
    experts, rows, cols = master.shape
    width = cols // n

    def source(d):
        return pl.BlockSpec((1, rows, width), lambda e, t: (first + e, 0, t[d]))

    def scale_of(d):
        return pl.BlockSpec((1, 1, width), lambda e, t: (offset + e, 0, t[d]))

    in_specs = [source(d) for d in range(n)] + [scale_of(d) for d in range(n)]
    args = [master] * n + [scale] * n
    aliases = {}
    if final is not None:
        in_specs.append(HBM)
        args.append(final)
        aliases = {1 + 2 * n: 0}
    piece = jax.ShapeDtypeStruct((count, rows, width), jnp.bfloat16)
    return pl.pallas_call(
        functools.partial(narrow_body, n),
        grid_spec=pltpu.PrefetchScalarGridSpec(
            num_scalar_prefetch=1,
            grid=(count,),
            in_specs=in_specs,
            out_specs=[pl.BlockSpec((1, rows, width), lambda e, t: (first + e, t[0], 0))]
            + [pl.BlockSpec((1, rows, width), lambda e, t: (e, 0, 0)) for _ in range(n - 1)],
        ),
        out_shape=[jax.ShapeDtypeStruct((experts, rows * n, width), jnp.bfloat16)] + [piece] * (n - 1),
        input_output_aliases=aliases,
        name="narrow",
    )(targets, *args)


def spread_direct(value, n):
    got = [swap(value, "shard", n, d) for d in range(n - 1, 0, -1)]
    return functools.reduce(jnp.maximum, got, value)


def spread_doubling(value, n):
    step = 1
    while step < n:
        value = jnp.maximum(value, swap(value, "shard", n, step))
        step *= 2
    return value


def router(weight, gain, n, m):
    part = (weight * gain[:, None]).astype(jnp.bfloat16).T
    experts, rows = part.shape
    mine = lax.axis_index("shard")
    tall = jnp.zeros((experts, rows * n), part.dtype)
    held = part
    step = n // 2
    while step:
        got = swap(held, "shard", n, step)
        held = jnp.concatenate([held, got], axis=1)
        step //= 2
    order = [0]
    step = n // 2
    while step:
        order += [k ^ step for k in order]
        step //= 2
    for k, d in enumerate(order):
        piece = held[:, k * rows : (k + 1) * rows]
        tall = lax.dynamic_update_slice_in_dim(tall, piece, (mine ^ d) * rows, 1)
    mine = lax.axis_index("expert")
    full = jnp.zeros((experts * m, rows * n), part.dtype)
    for d in range(m):
        got = tall if d == 0 else swap(tall, "expert", m, d)
        full = lax.dynamic_update_slice_in_dim(full, got, (mine ^ d) * experts, 0)
    return full.T


def own_columns(scale, n):
    width = scale.shape[1] // n
    return lax.dynamic_slice_in_dim(scale, lax.axis_index("shard") * width, width, axis=1)


def plain(master_gate, master_up, router_weight, router_gain, n):
    scales = lax.pmax(
        (jnp.max(jnp.abs(master_gate), axis=1), jnp.max(jnp.abs(master_up), axis=1)), "shard"
    )
    finals = [
        lax.all_to_all(
            (master / jnp.expand_dims(scale, 1)).astype(jnp.bfloat16), "shard", split_axis=2, concat_axis=1, tiled=True
        )
        for master, scale in zip((master_gate, master_up), scales)
    ]
    part = (router_weight * router_gain[:, None]).astype(jnp.bfloat16)
    part = lax.all_gather(part, "shard", axis=0, tiled=True)
    part = lax.all_gather(part, "expert", axis=1, tiled=True)
    return (*finals, *(own_columns(scale, n) for scale in scales), part)


def shards(n, m, master_gate, master_up, router_weight, router_gain):
    experts, rows, cols = master_gate.shape
    if n & (n - 1) or m & (m - 1) or n == 1 or cols % (n * LANES) or rows % 16 or experts % 16:
        return plain(master_gate, master_up, router_weight, router_gain, n)
    mine = lax.axis_index("shard")
    targets = jnp.stack([mine ^ d for d in range(n)]).astype(jnp.int32)
    masters = (master_gate, master_up)
    unit = experts // 16
    lead = 5 * unit
    plan = [(t, first * unit, count * unit) for t, first, count in PLAN]

    head = spread_direct(peaks(master_gate, 0, lead), n)
    finals = [None, None]
    sent = []
    tail_scales = [None, None]
    for k, (tensor, first, count) in enumerate(plan):
        if k < LEAD:
            scale, offset = head, first
        else:
            scale, offset = tail_scales[tensor], first - (lead if tensor == 0 else 0)
        finals[tensor], *pieces = narrow(masters[tensor], scale, targets, first, count, offset, n, finals[tensor])
        if k == LEAD - 1:
            rest_gate = peaks(master_gate, lead, experts - lead, pieces)
            rest_up = peaks(master_up, 0, experts, pieces)
            rest = spread_doubling(jnp.concatenate([rest_gate, rest_up], axis=0), n)
            tail_scales = [rest[: experts - lead], rest[experts - lead :]]
        sent.append([(d, swap(pieces[d - 1], "shard", n, d)) for d in range(n - 1, 0, -1)])
    for (tensor, first, count), got in zip(plan, sent):
        for d, piece in got[-1:] + got[:-1]:
            finals[tensor] = lax.dynamic_update_slice(finals[tensor], piece, (first, (mine ^ d) * rows, 0))
    scale_gate = jnp.concatenate([head, tail_scales[0]], axis=0)[:, 0]
    scale_up = tail_scales[1][:, 0]
    serve_router = router(router_weight, router_gain, n, m)
    return (*finals, own_columns(scale_gate, n), own_columns(scale_up, n), serve_router)


def solution(mesh):
    in_specs = (
        P(("shift", "expert"), "shard", None),
        P(("shift", "expert"), "shard", None),
        P(("shift", "shard"), "expert"),
        P(("shift", "shard")),
    )
    out_specs = (
        P(("shift", "expert"), None, "shard"),
        P(("shift", "expert"), None, "shard"),
        P(("shift", "expert"), "shard"),
        P(("shift", "expert"), "shard"),
        P("shift", None),
    )
    body = functools.partial(shards, mesh.shape["shard"], mesh.shape["expert"])

    return jax.shard_map(body, mesh=mesh, in_specs=in_specs, out_specs=out_specs, check_vma=False)
```

```python
import functools

import jax
import jax.numpy as jnp
from jax import lax
from jax.experimental import pallas as pl
from jax.experimental.pallas import tpu as pltpu
from jax.sharding import PartitionSpec as P

LANES = 128
PLAN = [(0, 0, 1), (0, 1, 2), (0, 3, 1), (0, 4, 3), (0, 7, 9), (1, 0, 8), (1, 8, 7), (1, 15, 1)]
LEAD = 3
HBM = pl.BlockSpec(memory_space=pl.ANY)


def swap(value, axis, size, step):
    return lax.ppermute(value, axis, [(i, i ^ step) for i in range(size)])


def peak_body(*refs):
    refs[-1][...] = jnp.max(jnp.abs(refs[0][...]), axis=1, keepdims=True)


def peaks(master, first, count, after=()):
    _, rows, cols = master.shape
    group = 2 if first % 2 == 0 and count % 2 == 0 else 1
    return pl.pallas_call(
        peak_body,
        grid=(count // group,),
        in_specs=[pl.BlockSpec((group, rows, cols), lambda e: (first // group + e, 0, 0))] + [HBM] * len(after),
        out_specs=pl.BlockSpec((group, 1, cols), lambda e: (e, 0, 0)),
        out_shape=jax.ShapeDtypeStruct((count, 1, cols), jnp.float32),
        name="peaks",
    )(master, *after)


def narrow_body(n, targets, *refs):
    outs = refs[-n:]
    for d in range(n):
        outs[d][0] = (refs[d][0] / refs[n + d][0]).astype(jnp.bfloat16)


def narrow(master, scale, targets, first, count, offset, n, cuts, final=None):
    experts, rows, cols = master.shape
    width = cols // n
    block = (1, rows // cuts, width)

    def source(d):
        return pl.BlockSpec(block, lambda e, r, t: (first + e, r, t[d]))

    def scale_of(d):
        return pl.BlockSpec((1, 1, width), lambda e, r, t: (offset + e, 0, t[d]))

    in_specs = [source(d) for d in range(n)] + [scale_of(d) for d in range(n)]
    args = [master] * n + [scale] * n
    aliases = {}
    if final is not None:
        in_specs.append(HBM)
        args.append(final)
        aliases = {1 + 2 * n: 0}
    piece = jax.ShapeDtypeStruct((count, rows, width), jnp.bfloat16)
    return pl.pallas_call(
        functools.partial(narrow_body, n),
        grid_spec=pltpu.PrefetchScalarGridSpec(
            num_scalar_prefetch=1,
            grid=(count, cuts),
            in_specs=in_specs,
            out_specs=[pl.BlockSpec(block, lambda e, r, t: (first + e, t[0] * cuts + r, 0))]
            + [pl.BlockSpec(block, lambda e, r, t: (e, r, 0)) for _ in range(n - 1)],
        ),
        out_shape=[jax.ShapeDtypeStruct((experts, rows * n, width), jnp.bfloat16)] + [piece] * (n - 1),
        input_output_aliases=aliases,
        name="narrow",
    )(targets, *args)


def spread_direct(value, n):
    got = [swap(value, "shard", n, d) for d in range(n - 1, 0, -1)]
    return functools.reduce(jnp.maximum, got, value)


def spread_doubling(value, n):
    step = 1
    while step < n:
        value = jnp.maximum(value, swap(value, "shard", n, step))
        step *= 2
    return value


def router(weight, gain, n, m):
    part = (weight * gain[:, None]).astype(jnp.bfloat16).T
    experts, rows = part.shape
    mine = lax.axis_index("shard")
    tall = jnp.zeros((experts, rows * n), part.dtype)
    held = part
    step = n // 2
    while step:
        got = swap(held, "shard", n, step)
        held = jnp.concatenate([held, got], axis=1)
        step //= 2
    order = [0]
    step = n // 2
    while step:
        order += [k ^ step for k in order]
        step //= 2
    for k, d in enumerate(order):
        piece = held[:, k * rows : (k + 1) * rows]
        tall = lax.dynamic_update_slice_in_dim(tall, piece, (mine ^ d) * rows, 1)
    mine = lax.axis_index("expert")
    full = jnp.zeros((experts * m, rows * n), part.dtype)
    for d in range(m):
        got = tall if d == 0 else swap(tall, "expert", m, d)
        full = lax.dynamic_update_slice_in_dim(full, got, (mine ^ d) * experts, 0)
    return full.T


def own_columns(scale, n):
    width = scale.shape[1] // n
    return lax.dynamic_slice_in_dim(scale, lax.axis_index("shard") * width, width, axis=1)


def plain(master_gate, master_up, router_weight, router_gain, n):
    scales = lax.pmax(
        (jnp.max(jnp.abs(master_gate), axis=1), jnp.max(jnp.abs(master_up), axis=1)), "shard"
    )
    finals = [
        lax.all_to_all(
            (master / jnp.expand_dims(scale, 1)).astype(jnp.bfloat16), "shard", split_axis=2, concat_axis=1, tiled=True
        )
        for master, scale in zip((master_gate, master_up), scales)
    ]
    part = (router_weight * router_gain[:, None]).astype(jnp.bfloat16)
    part = lax.all_gather(part, "shard", axis=0, tiled=True)
    part = lax.all_gather(part, "expert", axis=1, tiled=True)
    return (*finals, *(own_columns(scale, n) for scale in scales), part)


def shards(n, m, master_gate, master_up, router_weight, router_gain):
    experts, rows, cols = master_gate.shape
    if n & (n - 1) or m & (m - 1) or n == 1 or cols % (n * LANES) or rows % 64 or experts % 16:
        return plain(master_gate, master_up, router_weight, router_gain, n)
    mine = lax.axis_index("shard")
    targets = jnp.stack([mine ^ d for d in range(n)]).astype(jnp.int32)
    masters = (master_gate, master_up)
    unit = experts // 16
    lead = PLAN[LEAD][1] * unit
    plan = [(t, first * unit, count * unit) for t, first, count in PLAN]

    head = spread_direct(peaks(master_gate, 0, lead), n)
    finals = [None, None]
    sent = []
    tail_scales = [None, None]
    for k, (tensor, first, count) in enumerate(plan):
        if k < LEAD:
            scale, offset = head, first
        else:
            scale, offset = tail_scales[tensor], first - (lead if tensor == 0 else 0)
        finals[tensor], *pieces = narrow(masters[tensor], scale, targets, first, count, offset, n, 1, finals[tensor])
        if k == LEAD - 2:
            rest_gate = peaks(master_gate, lead, experts - lead, after=pieces)
            rest_up = peaks(master_up, 0, experts, after=pieces)
            rest = spread_doubling(jnp.concatenate([rest_gate, rest_up], axis=0), n)
            tail_scales = [rest[: experts - lead], rest[experts - lead :]]
        sent.append([(d, swap(pieces[d - 1], "shard", n, d)) for d in range(n - 1, 0, -1)])
    for (tensor, first, count), got in zip(plan, sent):
        for d, piece in got[-1:] + got[:-1]:
            finals[tensor] = lax.dynamic_update_slice(finals[tensor], piece, (first, (mine ^ d) * rows, 0))
    scale_gate = jnp.concatenate([head, tail_scales[0]], axis=0)[:, 0]
    scale_up = tail_scales[1][:, 0]
    serve_router = router(router_weight, router_gain, n, m)
    return (*finals, own_columns(scale_gate, n), own_columns(scale_up, n), serve_router)


def solution(mesh):
    in_specs = (
        P(("shift", "expert"), "shard", None),
        P(("shift", "expert"), "shard", None),
        P(("shift", "shard"), "expert"),
        P(("shift", "shard")),
    )
    out_specs = (
        P(("shift", "expert"), None, "shard"),
        P(("shift", "expert"), None, "shard"),
        P(("shift", "expert"), "shard"),
        P(("shift", "expert"), "shard"),
        P("shift", None),
    )
    body = functools.partial(shards, mesh.shape["shard"], mesh.shape["expert"])

    return jax.shard_map(body, mesh=mesh, in_specs=in_specs, out_specs=out_specs, check_vma=False)
```
